256 devices in a mesh: lat: 16 (over y, x_hi, core), lon: 16 (over x_lo, z).
Axes of the slice: x: 4 (x_hi: 2, x_lo: 2; x = x_hi * 2 + x_lo), y: 4, z: 8, core: 2. Of those that a mesh axis runs over, the one named last changes fastest.
Arguments:
- inputs: bfloat16 [256, 1536, 256], P('lat', 'lon'), may hold values from -6 to 6
- first_filter: bfloat16 [3, 3, 256, 256], replicated, may hold values from -0.125 to 0.125
- second_filter: bfloat16 [3, 3, 256, 256], replicated, may hold values from -0.125 to 0.125
- cotangent: bfloat16 [256, 1536, 256], P('lat', 'lon'), may hold values from -30 to 30
Outputs:
- input_grad: bfloat16 [256, 1536, 256], P('lat', 'lon')
- first_grad: float32 [3, 3, 256, 256], replicated
- second_grad: float32 [3, 3, 256, 256], replicated
The draws below stay inside these ranges and needn't reach their ends.
All inputs are finite; a program needn't handle non-finite values.
Results may differ from the reference program's by a relative error of at most 0.0061.
Values may be sent and summed in bfloat16 or wider, within the bound.
A program may use at most 64 MiB of HBM per device.

```python
import jax
import jax.numpy as jnp
from jax import lax

CH = 256
NLAT = 256
NLON = 1536


def draw_cotangent(key, part):
    lat_pos = jnp.arange(NLAT, dtype=jnp.float32)[:, None, None] / NLAT
    lon_pos = jnp.arange(NLON, dtype=jnp.float32)[None, :, None] / NLON
    rough = jax.random.uniform(jax.random.fold_in(key, 7), (NLAT, NLON, 1), jnp.float32, 0.5, 1.5)
    base = jnp.clip(jax.random.normal(key, (NLAT, NLON, CH), jnp.float32), -6.0, 6.0)
    scale = jnp.exp(jnp.log(3.0) * (lat_pos + lon_pos))
    return jnp.clip(base * rough * scale / 3.0, -30.0, 30.0).astype(jnp.bfloat16)


def levels(stream_key, shape, pieces, low, top_value):
    def one(position, shards_of):
        steps = jax.random.uniform(jax.random.fold_in(jax.random.fold_in(stream_key, 6), position), (shards_of,), jnp.float32, low / len(pieces), top_value / len(pieces))
        return jnp.repeat(jnp.exp(steps), shape[position] // shards_of).reshape((-1,) + (1,) * (len(shape) - position - 1))

    level = one(*pieces[0])
    for cut in pieces[1:]:
        level = level * one(*cut)
    return level


def gaussian(stream_key, extent, deviation, reach, cuts=(), kind=jnp.bfloat16):
    result = jax.random.normal(stream_key, extent, jnp.float32) * deviation
    if len(cuts) > 0:
        result = levels(stream_key, extent, cuts, -0.22, 0.18) * result
    return jnp.clip(result, min=-reach, max=reach).astype(kind)


def setup_inputs(seed: int = 0) -> dict:
    keys = jax.random.split(jax.random.key(seed), 5)
    return {
        "inputs": gaussian(keys[0], (NLAT, NLON, CH), 1.0, 6.0, ((0, 16), (1, 16))),
        "first_filter": gaussian(keys[1], (3, 3, CH, CH), (9 * CH) ** -0.5, 0.125),
        "second_filter": gaussian(keys[2], (3, 3, CH, CH), (9 * CH) ** -0.5, 0.125),
        "cotangent": draw_cotangent(jax.random.fold_in(keys[4], 71), 0),
    }


def pad_field(field):
    wrapped = jnp.concatenate([field[:, -1:], field, field[:, :1]], axis=1)
    zeros = jnp.zeros((1,) + wrapped.shape[1:], wrapped.dtype)
    return jnp.concatenate([zeros, wrapped, zeros], axis=0)

def conv_taps(padded, weight, rows, cols, flipped):
    total = jnp.zeros((rows * cols, weight.shape[3] if not flipped else weight.shape[2]), jnp.float32)
    for first in range(3):
        for second in range(3):
            piece = padded[first:first + rows, second:second + cols, :].reshape(rows * cols, -1)
            if flipped:
                total = total + lax.dot_general(piece, weight[2 - first, 2 - second], (((1,), (1,)), ((), ())), preferred_element_type=jnp.float32)
            else:
                total = total + jnp.dot(piece, weight[first, second], preferred_element_type=jnp.float32)
    return total.reshape(rows, cols, -1)

def filter_grad(padded, delta, rows, cols):
    flat = delta.reshape(rows * cols, -1)
    taps = []
    for first in range(3):
        for second in range(3):
            piece = padded[first:first + rows, second:second + cols, :].reshape(rows * cols, -1)
            taps.append(lax.dot_general(piece, flat, (((0,), (0,)), ((), ())), preferred_element_type=jnp.float32))
    return jnp.stack(taps).reshape(3, 3, flat.shape[1], flat.shape[1])

def gelu_value(value):
    return value * 0.5 * (1.0 + jax.scipy.special.erf(value * 0.7071067811865476))

def gelu_slope(value):
    return 0.5 * (1.0 + jax.scipy.special.erf(value * 0.7071067811865476)) + value * jnp.exp(-0.5 * value * value) * 0.3989422804014327

def reference(inputs, first_filter, second_filter, cotangent):
    rows, cols = (inputs.shape[0], inputs.shape[1])
    padded_in = pad_field(inputs)
    hidden_one = conv_taps(padded_in, first_filter, rows, cols, False)
    act = gelu_value(hidden_one).astype(jnp.bfloat16)
    padded_act = pad_field(act)
    hidden_two = conv_taps(padded_act, second_filter, rows, cols, False)
    delta_two = (cotangent.astype(jnp.float32) * gelu_slope(hidden_two)).astype(jnp.bfloat16)
    second_grad = filter_grad(padded_act, delta_two, rows, cols)
    act_grad = conv_taps(pad_field(delta_two), second_filter, rows, cols, True)
    delta_one = (act_grad * gelu_slope(hidden_one)).astype(jnp.bfloat16)
    first_grad = filter_grad(padded_in, delta_one, rows, cols)
    input_grad = conv_taps(pad_field(delta_one), first_filter, rows, cols, True).astype(jnp.bfloat16)
    return (input_grad, first_grad, second_grad)
```

```python
import functools

import jax
import jax.numpy as jnp
from jax import lax
from jax.experimental import pallas as pl
from jax.experimental.pallas import tpu as pltpu
from jax.sharding import PartitionSpec as P

MESH = pl.DeviceIdType.MESH
F32 = jnp.float32
BF16 = jnp.bfloat16
VMEM_LIMIT = 60 * 1024 * 1024


def slope_parts(value):
    half = 0.5 * (1.0 + lax.erf(value * 0.7071067811865476))
    slope = half + value * jnp.exp(-0.5 * value * value) * 0.3989422804014327
    return half, slope


def stage_kernel(
    lats, lons, rows, cols, ch, group,
    in_ref, w1_ref, w2_ref, cot_ref,
    dx_ref, g1_ref, g2_ref,
    xs, acts, d2s, d1s, slope1, turned, edge, sent, got, halo, send_sem, recv_sem,
):
    lat, lon = lax.axis_index("lat"), lax.axis_index("lon")
    size = group * cols
    blocks = rows // group

    def spot(dlat, dlon):
        return {"lat": lax.rem(lat + dlat + lats, lats), "lon": lax.rem(lon + dlon + lons, lons)}

    barrier = pltpu.get_barrier_semaphore()
    for dlat in (-1, 0, 1):
        for dlon in (-1, 0, 1):
            if dlat or dlon:
                pl.semaphore_signal(barrier, inc=1, device_id=spot(dlat, dlon), device_id_type=MESH)
    pl.semaphore_wait(barrier, 8)

    def line(row):
        return pl.ds(pl.multiple_of(row * cols, cols), cols)

    def put_row(field, row, value):
        where = line(row)
        field[where, ch : 2 * ch] = value.astype(BF16)
        field[where, 0:ch] = pltpu.roll(value, 1, 0).astype(BF16)
        field[where, 2 * ch : 3 * ch] = pltpu.roll(value, cols - 1, 0).astype(BF16)
        edge[0, pl.ds(row - 1, 1), :] = value[0:1]
        edge[1, pl.ds(row - 1, 1), :] = value[cols - 1 : cols]

    def copies(index, field):
        mid = slice(ch, 2 * ch)
        plan = [
            (field.at[cols : 2 * cols, mid], field.at[(rows + 1) * cols : (rows + 2) * cols, mid], (-1, 0)),
            (field.at[rows * cols : (rows + 1) * cols, mid], field.at[0:cols, mid], (1, 0)),
        ]
        for dlat in (-1, 0, 1):
            plan.append((sent.at[index, 0], got.at[index, 1, 1 - dlat], (dlat, -1)))
            plan.append((sent.at[index, 1], got.at[index, 0, 1 - dlat], (dlat, 1)))
        return [
            pltpu.make_async_remote_copy(
                src_ref=src, dst_ref=dst,
                send_sem=send_sem.at[index, n], recv_sem=recv_sem.at[index, n],
                device_id=spot(*shift), device_id_type=MESH,
            )
            for n, (src, dst, shift) in enumerate(plan)
        ]

    def send(index, field):
        for side in range(2):
            sent[index, side] = edge[side].astype(BF16)
        for copy in copies(index, field):
            copy.start()

    up, down = lat > 0, lat < lats - 1

    def receive(index, field):
        for copy in copies(index, field):
            copy.wait()
        for side in range(2):
            halo[side, 8 : 8 + rows] = got[index, side, 1].astype(F32)
            halo[side, 7:8] = jnp.where(up, got[index, side, 0].astype(F32)[rows - 1 : rows], 0.0)
            halo[side, 8 + rows : 9 + rows] = jnp.where(down, got[index, side, 2].astype(F32)[0:1], 0.0)
        spots = lax.broadcasted_iota(jnp.int32, (16, ch), 0)

        def fix(row, carry):
            base = pl.multiple_of(row * cols, cols)
            head = pl.ds(base, 16)
            tail = pl.ds(pl.multiple_of(base + cols - 16, 16), 16)
            left = halo[0, pl.ds(7 + row, 1), :]
            right = halo[1, pl.ds(7 + row, 1), :]
            field[head, 0:ch] = jnp.where(spots == 0, left, field[head, 0:ch].astype(F32)).astype(BF16)
            field[tail, 2 * ch : 3 * ch] = jnp.where(
                spots == 15, right, field[tail, 2 * ch : 3 * ch].astype(F32)
            ).astype(BF16)
            return carry

        lax.fori_loop(1, rows + 1, fix, 0)
        place = lax.broadcasted_iota(jnp.int32, (cols, ch), 0)
        for row, valid in ((0, up), (rows + 1, down)):
            where = slice(row * cols, (row + 1) * cols)
            value = jnp.where(valid, field[where, ch : 2 * ch].astype(F32), 0.0)
            field[where, ch : 2 * ch] = value.astype(BF16)
            field[where, 0:ch] = jnp.where(
                place == 0, halo[0, 7 + row : 8 + row, :], pltpu.roll(value, 1, 0)
            ).astype(BF16)
            field[where, 2 * ch : 3 * ch] = jnp.where(
                place == cols - 1, halo[1, 7 + row : 8 + row, :], pltpu.roll(value, cols - 1, 0)
            ).astype(BF16)

    def conv(field, weight, block):
        total = None
        for a in range(3):
            piece = field[pl.ds(pl.multiple_of((block * group + a) * cols, cols), size), :]
            part = jnp.dot(piece, weight[a], preferred_element_type=F32)
            total = part if total is None else total + part
        return total

    def conv_t(field, weight, block):
        total = None
        for a in range(3):
            for b in range(3):
                piece = field[
                    pl.ds(pl.multiple_of((block * group + a) * cols, cols), size), b * ch : (b + 1) * ch
                ]
                part = lax.dot_general(
                    piece, weight[2 - a, (2 - b) * ch : (3 - b) * ch, :],
                    (((1,), (1,)), ((), ())), preferred_element_type=F32,
                )
                total = part if total is None else total + part
        return total

    def put_block(field, block, value):
        for k in range(group):
            put_row(field, block * group + 1 + k, value[k * cols : (k + 1) * cols])

    def filter_grad(field, grad):
        def tap(a, carry):
            grad[a] = jnp.dot(
                turned[...], field[pl.ds(pl.multiple_of(a * cols, cols), rows * cols), :],
                preferred_element_type=F32,
            )
            return carry

        lax.fori_loop(0, 3, tap, 0)

    def load(row, carry):
        put_row(xs, row + 1, in_ref[row].astype(F32))
        return carry

    lax.fori_loop(0, rows, load, 0)
    send(0, xs)
    receive(0, xs)

    def first(block, carry):
        value = conv(xs, w1_ref, block)
        half, slope = slope_parts(value)
        slope1[pl.ds(pl.multiple_of(block * size, size), size), :] = slope
        put_block(acts, block, value * half)
        return carry

    lax.fori_loop(0, blocks, first, 0)
    send(1, acts)
    receive(1, acts)

    def second(block, carry):
        value = conv(acts, w2_ref, block)
        _, slope = slope_parts(value)
        rate = cot_ref[pl.ds(block * group, group)].astype(F32).reshape(size, ch)
        delta = rate * slope
        put_block(d2s, block, delta)
        turned[:, pl.ds(pl.multiple_of(block * size, size), size)] = delta.T.astype(BF16)
        return carry

    lax.fori_loop(0, blocks, second, 0)
    send(2, d2s)
    filter_grad(acts, g2_ref)
    receive(2, d2s)

    def third(block, carry):
        value = conv_t(d2s, w2_ref, block)
        delta = value * slope1[pl.ds(pl.multiple_of(block * size, size), size), :]
        put_block(d1s, block, delta)
        turned[:, pl.ds(pl.multiple_of(block * size, size), size)] = delta.T.astype(BF16)
        return carry

    lax.fori_loop(0, blocks, third, 0)
    send(3, d1s)
    filter_grad(xs, g1_ref)
    receive(3, d1s)

    def fourth(block, carry):
        value = conv_t(d1s, w1_ref, block)
        dx_ref[pl.ds(block * group, group)] = value.astype(BF16).reshape(group, cols, ch)
        return carry

    lax.fori_loop(0, blocks, fourth, 0)


def reduce_kernel(
    ch, half,
    g1_ref, g2_ref, o1_ref, o2_ref,
    pair, mine, out1, in1, mine2, out2, in2, mine3, in3, final,
    pair_send, pair_recv, s1, r1, s2, r2, s3, r3, s4, r4, s5, r5, s6, r6, last_send, last_recv,
):
    lat, lon = lax.axis_index("lat"), lax.axis_index("lon")
    core = lax.rem(lat, 2)
    x = lax.rem(lat // 2, 2) * 2 + lon // 8
    y = lat // 4
    z = lax.rem(lon, 8)

    def at(x, y, z, core):
        return {"lat": y * 4 + (x // 2) * 2 + core, "lon": lax.rem(x, 2) * 8 + z}

    partner = at(x, y, z, 1 - core)

    def along_x(d):
        return at(lax.rem(x + d, 4), y, z, core)

    def along_y(d):
        return at(x, lax.rem(y + d, 4), z, core)

    def along_z(d):
        return at(x, y, lax.rem(z + d, 8), core)

    barrier = pltpu.get_barrier_semaphore()
    peers = [partner] + [along_x(d) for d in (1, 2, 3)] + [along_y(d) for d in (1, 2, 3)]
    peers += [along_z(d) for d in range(1, 8)]
    for peer in peers:
        pl.semaphore_signal(barrier, inc=1, device_id=peer, device_id_type=MESH)
    pl.semaphore_wait(barrier, len(peers))

    grads = (g1_ref, g2_ref)
    outs = (o1_ref, o2_ref)
    order = ((x, along_x, y, along_y), (y, along_y, x, along_x))

    def remote(src, dst, send_sem, recv_sem, device):
        return pltpu.make_async_remote_copy(
            src_ref=src, dst_ref=dst, send_sem=send_sem, recv_sem=recv_sem,
            device_id=device, device_id_type=MESH,
        )

    def rows64(index):
        return pl.ds(pl.multiple_of(index * 64, 64), 64)

    def rows16(index):
        return pl.ds(pl.multiple_of(index * 16, 16), 16)

    def pair_copy(g):
        other = pl.ds(pl.multiple_of((1 - core) * half, half), half)
        return remote(grads[g].at[:, other, :], pair.at[g], pair_send.at[g], pair_recv.at[g], partner)

    def first_copies(g):
        index, peer = order[g][:2]
        return [
            remote(
                out1.at[g, :, rows64(lax.rem(index + d, 4)), :], in1.at[g, d - 1],
                s1.at[g, d - 1], r1.at[g, d - 1], peer(d),
            )
            for d in (1, 2, 3)
        ]

    def second_copies(g):
        index, peer = order[g][2:]
        return [
            remote(
                out2.at[g, :, rows16(lax.rem(index + d, 4)), :], in2.at[g, d - 1],
                s2.at[g, d - 1], r2.at[g, d - 1], peer(d),
            )
            for d in (1, 2, 3)
        ]

    def third_copies(g):
        found = []
        for d in range(1, 8):
            found.append(
                remote(
                    mine3.at[g, lax.rem(z + d, 8)], in3.at[g, z, 0],
                    s3.at[g, d - 1, 0], r3.at[g, d - 1, 0], along_z(d),
                )
            )
            found.append(
                remote(
                    mine3.at[g, 8], in3.at[g, z, 1],
                    s3.at[g, d - 1, 1], r3.at[g, d - 1, 1], along_z(d),
                )
            )
        return found

    def chunk(g):
        return rows16(order[g][0] * 4 + order[g][2])

    def fourth_copies(g):
        place = final.at[g, core, z, chunk(g), :]
        return [
            remote(place, place, s4.at[g, d - 1], r4.at[g, d - 1], along_z(d)) for d in range(1, 8)
        ]

    def fifth_copies(g):
        place = final.at[g, core, :, chunk(g), :]
        return [
            remote(place, place, s5.at[g, d - 1], r5.at[g, d - 1], order[g][3](d)) for d in (1, 2, 3)
        ]

    def sixth_copies(g):
        place = final.at[g, core, :, rows64(order[g][0]), :]
        return [
            remote(place, place, s6.at[g, d - 1], r6.at[g, d - 1], order[g][1](d)) for d in (1, 2, 3)
        ]

    def last_copy(g):
        place = final.at[g, core]
        return remote(place, place, last_send.at[g], last_recv.at[g], partner)

    for g in range(2):
        pair_copy(g).start()
    for g in range(2):
        pair_copy(g).wait()
        own = pl.ds(pl.multiple_of(core * half, half), half)
        for b in range(3):
            def turn(a, carry):
                total = grads[g][a, own, b * ch : (b + 1) * ch] + pair[g, a, :, b * ch : (b + 1) * ch]
                total = total.T
                mine[g, a * 3 + b] = total
                out1[g, a * 3 + b] = total.astype(BF16)
                return carry

            lax.fori_loop(0, 3, turn, 0)
        for copy in first_copies(g):
            copy.start()
    for g in range(2):
        for copy in first_copies(g):
            copy.wait()

        def add_first(t, carry):
            total = mine[g, t, rows64(order[g][0]), :]
            for d in range(3):
                total = total + in1[g, d, t].astype(F32)
            mine2[g, t] = total
            out2[g, t] = total.astype(BF16)
            return carry

        lax.fori_loop(0, 9, add_first, 0)
        for copy in second_copies(g):
            copy.start()
    for g in range(2):
        for copy in second_copies(g):
            copy.wait()

        def add_second(t, carry):
            total = mine2[g, t, rows16(order[g][2]), :]
            for d in range(3):
                total = total + in2[g, d, t].astype(F32)
            mine3[g, t] = total
            return carry

        lax.fori_loop(0, 9, add_second, 0)
        in3[g, z, 0] = mine3[g, z]
        in3[g, z, 1] = mine3[g, 8]
        for copy in third_copies(g):
            copy.start()
    for g in range(2):
        for copy in third_copies(g):
            copy.wait()
        for k in range(2):
            total = in3[g, 0, k]
            for m in range(1, 8):
                total = total + in3[g, m, k]
            final[g, core, z if k == 0 else 8, chunk(g), :] = total.astype(BF16)
        for copy in fourth_copies(g):
            copy.start()
    for g in range(2):
        for copy in fourth_copies(g):
            copy.wait()
        for copy in fifth_copies(g):
            copy.start()
    for g in range(2):
        for copy in fifth_copies(g):
            copy.wait()
        for copy in sixth_copies(g):
            copy.start()
    for g in range(2):
        for copy in sixth_copies(g):
            copy.wait()
        last_copy(g).start()
    for g in range(2):
        last_copy(g).wait()

        def emit(t, carry):
            for c in range(2):
                outs[g][t, :, c * half : (c + 1) * half] = final[g, c, t].astype(F32)
            return carry

        lax.fori_loop(0, 9, emit, 0)


def body(lats, lons, inputs, first_filter, second_filter, cotangent):
    rows, cols, ch = inputs.shape
    group = 4
    vmem = pl.BlockSpec(memory_space=pltpu.VMEM)
    cells = rows * cols
    padded = pltpu.VMEM(((rows + 2) * cols, 3 * ch), BF16)
    dx, g1, g2 = pl.pallas_call(
        functools.partial(stage_kernel, lats, lons, rows, cols, ch, group),
        out_shape=(
            jax.ShapeDtypeStruct((rows, cols, ch), BF16),
            jax.ShapeDtypeStruct((3, ch, 3 * ch), F32),
            jax.ShapeDtypeStruct((3, ch, 3 * ch), F32),
        ),
        in_specs=[vmem] * 4,
        out_specs=(vmem,) * 3,
        scratch_shapes=[
            padded, padded, padded, padded,
            pltpu.VMEM((cells, ch), F32),
            pltpu.VMEM((ch, cells), BF16),
            pltpu.VMEM((2, rows, ch), F32),
            pltpu.VMEM((4, 2, rows, ch), BF16),
            pltpu.VMEM((4, 2, 3, rows, ch), BF16),
            pltpu.VMEM((2, 16 + rows, ch), F32),
            pltpu.SemaphoreType.DMA((4, 8)),
            pltpu.SemaphoreType.DMA((4, 8)),
        ],
        compiler_params=pltpu.CompilerParams(
            collective_id=0, has_side_effects=True, vmem_limit_bytes=VMEM_LIMIT
        ),
        name="stages",
    )(
        inputs,
        first_filter.reshape(3, 3 * ch, ch),
        second_filter.reshape(3, 3 * ch, ch),
        cotangent,
    )
    half = ch // 2
    dma = pltpu.SemaphoreType.DMA
    o1, o2 = pl.pallas_call(
        functools.partial(reduce_kernel, ch, half),
        out_shape=(jax.ShapeDtypeStruct((9, ch, ch), F32),) * 2,
        in_specs=[vmem] * 2,
        out_specs=(vmem,) * 2,
        scratch_shapes=[
            pltpu.VMEM((2, 3, half, 3 * ch), F32),
            pltpu.VMEM((2, 9, ch, half), F32),
            pltpu.VMEM((2, 9, ch, half), BF16),
            pltpu.VMEM((2, 3, 9, 64, half), BF16),
            pltpu.VMEM((2, 9, 64, half), F32),
            pltpu.VMEM((2, 9, 64, half), BF16),
            pltpu.VMEM((2, 3, 9, 16, half), BF16),
            pltpu.VMEM((2, 9, 16, half), F32),
            pltpu.VMEM((2, 8, 2, 16, half), F32),
            pltpu.VMEM((2, 2, 9, ch, half), BF16),
            dma((2,)), dma((2,)),
            dma((2, 3)), dma((2, 3)),
            dma((2, 3)), dma((2, 3)),
            dma((2, 7, 2)), dma((2, 7, 2)),
            dma((2, 7)), dma((2, 7)),
            dma((2, 3)), dma((2, 3)),
            dma((2, 3)), dma((2, 3)),
            dma((2,)), dma((2,)),
        ],
        compiler_params=pltpu.CompilerParams(
            collective_id=1, has_side_effects=True, vmem_limit_bytes=VMEM_LIMIT
        ),
        name="reduce",
    )(g1, g2)
    return dx, o1.reshape(3, 3, ch, ch), o2.reshape(3, 3, ch, ch)


def solution(mesh):
    in_specs = (P("lat", "lon", None), P(), P(), P("lat", "lon", None))
    out_specs = (P("lat", "lon", None), P(), P())
    step = functools.partial(body, mesh.shape["lat"], mesh.shape["lon"])
    return jax.shard_map(step, mesh=mesh, in_specs=in_specs, out_specs=out_specs, check_vma=False)
```

```python
import functools

import jax
import jax.numpy as jnp
from jax import lax
from jax.experimental import pallas as pl
from jax.experimental.pallas import tpu as pltpu
from jax.sharding import PartitionSpec as P

MESH = pl.DeviceIdType.MESH
F32 = jnp.float32
BF16 = jnp.bfloat16
VMEM_LIMIT = 56 * 1024 * 1024


def slope_parts(value):
    half = 0.5 * (1.0 + lax.erf(value * 0.7071067811865476))
    slope = half + value * jnp.exp(-0.5 * value * value) * 0.3989422804014327
    return half, slope


def kernel(
    lats, lons, rows, cols, ch, group,
    in_hbm, w1_hbm, w2_hbm, cot_hbm,
    dx_ref, o1_ref, o2_ref,
    in_ref, w1_ref, w2_ref, cot_ref,
    xs, acts, d2s, d1s, slope1, turned, edge, sent, got, halo,
    grads, pair, mine, out1, in1, zin, final,
    load_sem, send_sem, recv_sem,
    pair_sem, plane_sem, z_sem, spread_sem, last_sem,
):
    lat, lon = lax.axis_index("lat"), lax.axis_index("lon")
    core = lax.rem(lat, 2)
    x = lax.rem(lat // 2, 2) * 2 + lon // 8
    y = lat // 4
    z = lax.rem(lon, 8)
    size = group * cols
    blocks = rows // group
    half = ch // 2
    mid = slice(ch, 2 * ch)

    loads = [
        pltpu.make_async_copy(src, dst, load_sem.at[n])
        for n, (src, dst) in enumerate(
            ((in_hbm, in_ref), (w1_hbm, w1_ref), (cot_hbm, cot_ref), (w2_hbm, w2_ref))
        )
    ]
    for copy in loads:
        copy.start()

    def spot(dlat, dlon):
        return {"lat": lax.rem(lat + dlat + lats, lats), "lon": lax.rem(lon + dlon + lons, lons)}

    def at(x, y, z, core):
        return {"lat": y * 4 + (x // 2) * 2 + core, "lon": lax.rem(x, 2) * 8 + z}

    partner = at(x, y, z, 1 - core)
    plane = [(dx, dy) for dx in range(4) for dy in range(4) if dx or dy]

    def in_plane(dx, dy):
        return lax.rem(x + dx, 4), lax.rem(y + dy, 4)

    around = [(dlat, dlon) for dlat in (-1, 0, 1) for dlon in (-1, 0, 1) if dlat or dlon]
    peers = [spot(*shift) for shift in around] + [partner]
    peers += [at(*in_plane(*shift), z, core) for shift in plane]
    peers += [at(x, y, lax.rem(z + d, 8), core) for d in range(1, 8)]
    barrier = pltpu.get_barrier_semaphore()
    for peer in peers:
        pl.semaphore_signal(barrier, inc=1, device_id=peer, device_id_type=MESH)

    def remote(src, dst, sems, device):
        return pltpu.make_async_remote_copy(
            src_ref=src, dst_ref=dst, send_sem=sems.at[0], recv_sem=sems.at[1],
            device_id=device, device_id_type=MESH,
        )

    def put_row(field, row, value, mark=True):
        where = pl.ds(pl.multiple_of(row * cols, cols), cols)
        field[where, mid] = value.astype(BF16)
        field[where, 0:ch] = pltpu.roll(value, 1, 0).astype(BF16)
        field[where, 2 * ch : 3 * ch] = pltpu.roll(value, cols - 1, 0).astype(BF16)
        if mark:
            edge[0, pl.ds(row - 1, 1), :] = value[0:1]
            edge[1, pl.ds(row - 1, 1), :] = value[cols - 1 : cols]

    def copies(index, field, which):
        if index == 0:
            first, last = in_ref.at[0], in_ref.at[rows - 1]
        else:
            first = field.at[cols : 2 * cols, mid]
            last = field.at[rows * cols : (rows + 1) * cols, mid]
        plan = [
            (first, field.at[(rows + 1) * cols : (rows + 2) * cols, mid], (-1, 0)),
            (last, field.at[0:cols, mid], (1, 0)),
        ]
        for dlat in (-1, 1, 0):
            plan.append((sent.at[index, 0], got.at[index, 1, 1 - dlat], (dlat, -1)))
            plan.append((sent.at[index, 1], got.at[index, 0, 1 - dlat], (dlat, 1)))
        return [
            pltpu.make_async_remote_copy(
                src_ref=plan[n][0], dst_ref=plan[n][1],
                send_sem=send_sem.at[index, n], recv_sem=recv_sem.at[index, n],
                device_id=spot(*plan[n][2]), device_id_type=MESH,
            )
            for n in which
        ]

    def send(index, field):
        for side in range(2):
            sent[index, side] = edge[side].astype(BF16)
        for copy in copies(index, field, range(8)):
            copy.start()

    up, down = lat > 0, lat < lats - 1

    def receive_sides(index, field):
        for copy in copies(index, field, (6, 7)):
            copy.wait()
        for side in range(2):
            halo[side, 8 : 8 + rows] = got[index, side, 1].astype(F32)
        spots = lax.broadcasted_iota(jnp.int32, (16, ch), 0)
        for row in range(1, rows + 1):
            head = slice(row * cols, row * cols + 16)
            tail = slice((row + 1) * cols - 16, (row + 1) * cols)
            left = halo[0, 7 + row : 8 + row, :]
            right = halo[1, 7 + row : 8 + row, :]
            field[head, 0:ch] = jnp.where(spots == 0, left, field[head, 0:ch].astype(F32)).astype(BF16)
            field[tail, 2 * ch : 3 * ch] = jnp.where(
                spots == 15, right, field[tail, 2 * ch : 3 * ch].astype(F32)
            ).astype(BF16)

    def receive_ends(index, field):
        for copy in copies(index, field, range(6)):
            copy.wait()
        place = lax.broadcasted_iota(jnp.int32, (cols, ch), 0)
        for row, valid, slot, pick in ((0, up, 0, rows - 1), (rows + 1, down, 2, 0)):
            where = slice(row * cols, (row + 1) * cols)
            value = jnp.where(valid, field[where, mid].astype(F32), 0.0)
            left, right = (
                jnp.where(valid, got[index, side, slot].astype(F32)[pick : pick + 1], 0.0)
                for side in range(2)
            )
            field[where, mid] = value.astype(BF16)
            field[where, 0:ch] = jnp.where(place == 0, left, pltpu.roll(value, 1, 0)).astype(BF16)
            field[where, 2 * ch : 3 * ch] = jnp.where(
                place == cols - 1, right, pltpu.roll(value, cols - 1, 0)
            ).astype(BF16)

    def conv(field, weight, block):
        total = None
        for a in range(3):
            piece = field[pl.ds(pl.multiple_of((block * group + a) * cols, cols), size), :]
            part = jnp.dot(piece, weight[a], preferred_element_type=F32)
            total = part if total is None else total + part
        return total

    def conv_t(field, weight, block):
        total = None
        for a in range(3):
            for b in range(3):
                piece = field[
                    pl.ds(pl.multiple_of((block * group + a) * cols, cols), size), b * ch : (b + 1) * ch
                ]
                part = lax.dot_general(
                    piece, weight[2 - a, (2 - b) * ch : (3 - b) * ch, :],
                    (((1,), (1,)), ((), ())), preferred_element_type=F32,
                )
                total = part if total is None else total + part
        return total

    def put_block(field, block, value):
        for k in range(group):
            put_row(field, block * group + 1 + k, value[k * cols : (k + 1) * cols])

    def stage(index, field, step):
        receive_sides(index, field)
        lax.fori_loop(1, blocks - 1, step, 0)
        receive_ends(index, field)
        lax.fori_loop(0, 2, lambda i, carry: step(i * (blocks - 1), carry), 0)

    own_rows = pl.ds(pl.multiple_of(core * half, half), half)
    other_rows = pl.ds(pl.multiple_of((1 - core) * half, half), half)

    def chunk(px, py):
        return pl.ds(pl.multiple_of((px * 4 + py) * 16, 16), 16)

    my_chunk = chunk(x, y)

    def taps(a):
        return slice(3 * a, 3 * a + 3)

    def pair_copy(g, a):
        return remote(grads.at[g, a, other_rows, :], pair.at[g, a], pair_sem.at[g, a], partner)

    def settle(ref, sems):
        pltpu.make_async_copy(ref, ref, sems.at[0]).wait()
        pltpu.make_async_copy(ref, ref, sems.at[1]).wait()

    def grad_piece(g, a, field):
        grads[g, a] = jnp.dot(
            turned[...], field[a * cols : (a + rows) * cols, :], preferred_element_type=F32
        )
        pair_copy(g, a).start()

    def scatter(g, a):
        pair_copy(g, a).wait()
        for b in range(3):
            lanes = slice(b * ch, (b + 1) * ch)
            total = (grads[g, a, own_rows, lanes] + pair[g, a, :, lanes]).T
            mine[g, a * 3 + b] = total
            out1[g, a * 3 + b] = total.astype(BF16)
        for n, shift in enumerate(plane):
            px, py = in_plane(*shift)
            remote(
                out1.at[g, taps(a), chunk(px, py), :], in1.at[g, a, n],
                plane_sem.at[g, a], at(px, py, z, core),
            ).start()

    def depth(g, a):
        settle(in1.at[g, a], plane_sem.at[g, a])
        total = mine[g, taps(a), my_chunk, :]
        for n in range(15):
            total = total + in1[g, a, n].astype(F32)
        zin[g, a, z] = total.astype(BF16)
        for d in range(1, 8):
            remote(
                zin.at[g, a, z], zin.at[g, a, z], z_sem.at[g, a],
                at(x, y, lax.rem(z + d, 8), core),
            ).start()

    def spread(g, a):
        settle(zin.at[g, a, 0:7], z_sem.at[g, a])
        total = zin[g, a, 0].astype(F32)
        for n in range(1, 8):
            total = total + zin[g, a, n].astype(F32)
        final[g, core, taps(a), my_chunk, :] = total.astype(BF16)
        place = final.at[g, core, taps(a), my_chunk, :]
        for shift in plane:
            px, py = in_plane(*shift)
            remote(place, place, spread_sem.at[g, a], at(px, py, z, core)).start()

    def last_copy(g, a):
        place = final.at[g, core, taps(a)]
        return remote(place, place, last_sem.at[g, a], partner)

    def join(g, a):
        settle(in1.at[g, a], spread_sem.at[g, a])
        last_copy(g, a).start()

    def finish(g, a):
        last_copy(g, a).wait()
        out = (o2_ref, o1_ref)[g]
        for c in range(2):
            out[taps(a), :, c * half : (c + 1) * half] = final[g, c, taps(a)]

    loads[0].wait()
    for row in range(rows):
        edge[0, row : row + 1] = in_ref[row, 0:16].astype(F32)[0:1]
        edge[1, row : row + 1] = in_ref[row, cols - 16 : cols].astype(F32)[15:16]
    pl.semaphore_wait(barrier, len(peers))
    send(0, xs)

    def load(row, carry):
        put_row(xs, row + 1, in_ref[row].astype(F32), mark=False)
        return carry

    lax.fori_loop(0, rows, load, 0)
    loads[1].wait()

    def first(block, carry):
        value = conv(xs, w1_ref, block)
        part, slope = slope_parts(value)
        slope1[pl.ds(pl.multiple_of(block * size, size), size), :] = slope
        put_block(acts, block, value * part)
        return carry

    stage(0, xs, first)
    send(1, acts)
    loads[2].wait()
    loads[3].wait()

    def second(block, carry):
        value = conv(acts, w2_ref, block)
        _, slope = slope_parts(value)
        rate = cot_ref[pl.ds(block * group, group)].astype(F32).reshape(size, ch)
        delta = rate * slope
        put_block(d2s, block, delta)
        turned[:, pl.ds(pl.multiple_of(block * size, size), size)] = delta.T.astype(BF16)
        return carry

    stage(1, acts, second)
    send(2, d2s)
    grad_piece(0, 0, acts)
    grad_piece(0, 1, acts)
    scatter(0, 0)
    grad_piece(0, 2, acts)
    scatter(0, 1)
    scatter(0, 2)

    def third(block, carry):
        value = conv_t(d2s, w2_ref, block)
        delta = value * slope1[pl.ds(pl.multiple_of(block * size, size), size), :]
        put_block(d1s, block, delta)
        turned[:, pl.ds(pl.multiple_of(block * size, size), size)] = delta.T.astype(BF16)
        return carry

    stage(2, d2s, third)
    send(3, d1s)
    grad_piece(1, 0, xs)
    grad_piece(1, 1, xs)
    scatter(1, 0)
    grad_piece(1, 2, xs)
    scatter(1, 1)
    scatter(1, 2)
    depth(0, 0)
    depth(0, 1)

    def fourth(block, carry):
        value = conv_t(d1s, w1_ref, block)
        dx_ref[pl.ds(block * group, group)] = value.astype(BF16).reshape(group, cols, ch)
        return carry

    receive_sides(3, d1s)
    lax.fori_loop(1, blocks - 1, fourth, 0)
    depth(0, 2)
    receive_ends(3, d1s)
    lax.fori_loop(0, 2, lambda i, carry: fourth(i * (blocks - 1), carry), 0)
    depth(1, 0)
    spread(0, 0)
    depth(1, 1)
    spread(0, 1)
    depth(1, 2)
    spread(0, 2)
    spread(1, 0)
    join(0, 0)
    spread(1, 1)
    join(0, 1)
    spread(1, 2)
    join(0, 2)
    finish(0, 0)
    finish(0, 1)
    finish(0, 2)
    join(1, 0)
    join(1, 1)
    finish(1, 0)
    join(1, 2)
    finish(1, 1)
    finish(1, 2)


def body(lats, lons, inputs, first_filter, second_filter, cotangent):
    rows, cols, ch = inputs.shape
    group = 4
    vmem = pl.BlockSpec(memory_space=pltpu.VMEM)
    hbm = pl.BlockSpec(memory_space=pl.ANY)
    cells = rows * cols
    half = ch // 2
    padded = pltpu.VMEM(((rows + 2) * cols, 3 * ch), BF16)
    dma = pltpu.SemaphoreType.DMA
    dx, o1, o2 = pl.pallas_call(
        functools.partial(kernel, lats, lons, rows, cols, ch, group),
        out_shape=(
            jax.ShapeDtypeStruct((rows, cols, ch), BF16),
            jax.ShapeDtypeStruct((9, ch, ch), BF16),
            jax.ShapeDtypeStruct((9, ch, ch), BF16),
        ),
        in_specs=[hbm] * 4,
        out_specs=(vmem,) * 3,
        scratch_shapes=[
            pltpu.VMEM((rows, cols, ch), BF16),
            pltpu.VMEM((3, 3 * ch, ch), BF16),
            pltpu.VMEM((3, 3 * ch, ch), BF16),
            pltpu.VMEM((rows, cols, ch), BF16),
            padded, padded, padded, padded,
            pltpu.VMEM((cells, ch), F32),
            pltpu.VMEM((ch, cells), BF16),
            pltpu.VMEM((2, rows, ch), F32),
            pltpu.VMEM((4, 2, rows, ch), BF16),
            pltpu.VMEM((4, 2, 3, rows, ch), BF16),
            pltpu.VMEM((2, 16 + rows, ch), F32),
            pltpu.VMEM((2, 3, ch, 3 * ch), F32),
            pltpu.VMEM((2, 3, half, 3 * ch), F32),
            pltpu.VMEM((2, 9, ch, half), F32),
            pltpu.VMEM((2, 9, ch, half), BF16),
            pltpu.VMEM((2, 3, 15, 3, 16, half), BF16),
            pltpu.VMEM((2, 3, 8, 3, 16, half), BF16),
            pltpu.VMEM((2, 2, 9, ch, half), BF16),
            dma((4,)), dma((4, 8)), dma((4, 8)),
            dma((2, 3, 2)), dma((2, 3, 2)), dma((2, 3, 2)), dma((2, 3, 2)), dma((2, 3, 2)),
        ],
        compiler_params=pltpu.CompilerParams(
            collective_id=0, has_side_effects=True, vmem_limit_bytes=VMEM_LIMIT
        ),
        name="stages",
    )(
        inputs,
        first_filter.reshape(3, 3 * ch, ch),
        second_filter.reshape(3, 3 * ch, ch),
        cotangent,
    )
    return dx, o1.astype(F32).reshape(3, 3, ch, ch), o2.astype(F32).reshape(3, 3, ch, ch)


def solution(mesh):
    in_specs = (P("lat", "lon", None), P(), P(), P("lat", "lon", None))
    out_specs = (P("lat", "lon", None), P(), P())
    step = functools.partial(body, mesh.shape["lat"], mesh.shape["lon"])
    return jax.shard_map(step, mesh=mesh, in_specs=in_specs, out_specs=out_specs, check_vma=False)
```

```python
import functools

import jax
import jax.numpy as jnp
from jax import lax
from jax.experimental import pallas as pl
from jax.experimental.pallas import tpu as pltpu
from jax.sharding import PartitionSpec as P

MESH = pl.DeviceIdType.MESH
F32 = jnp.float32
BF16 = jnp.bfloat16
VMEM_LIMIT = 44 * 1024 * 1024
MID = 4


def slope_parts(value):
    half = 0.5 * (1.0 + lax.erf(value * 0.7071067811865476))
    slope = half + value * jnp.exp(-0.5 * value * value) * 0.3989422804014327
    return half, slope


def kernel(
    lats, lons, rows, cols, ch, group,
    in_hbm, w1_hbm, w2_hbm, cot_hbm,
    dx_ref, o1_ref, o2_ref,
    in_ref, w1_ref, w2_ref, cot_ref,
    xs, acts, d2s, d1s, slope1, turned, edge, sent, got, halo,
    grads, pair, mine, out1, in1, zin, final,
    load_sem, send_sem, recv_sem,
    pair_sem, plane_sem, z_sem, spread_sem, last_sem,
):
    lat, lon = lax.axis_index("lat"), lax.axis_index("lon")
    core = lax.rem(lat, 2)
    x = lax.rem(lat // 2, 2) * 2 + lon // 8
    y = lat // 4
    z = lax.rem(lon, 8)
    size = group * cols
    half = ch // 2
    mid = slice(ch, 2 * ch)

    loads = [
        pltpu.make_async_copy(src, dst, load_sem.at[n])
        for n, (src, dst) in enumerate(
            ((in_hbm, in_ref), (w1_hbm, w1_ref), (cot_hbm, cot_ref), (w2_hbm, w2_ref))
        )
    ]
    for copy in loads:
        copy.start()

    def spot(dlat, dlon):
        return {"lat": lax.rem(lat + dlat + lats, lats), "lon": lax.rem(lon + dlon + lons, lons)}

    def at(x, y, z, core):
        return {"lat": y * 4 + (x // 2) * 2 + core, "lon": lax.rem(x, 2) * 8 + z}

    partner = at(x, y, z, 1 - core)
    plane = [(dx, dy) for dx in range(4) for dy in range(4) if dx or dy]

    def in_plane(dx, dy):
        return lax.rem(x + dx, 4), lax.rem(y + dy, 4)

    around = [(dlat, dlon) for dlat in (-1, 0, 1) for dlon in (-1, 0, 1) if dlat or dlon]
    peers = [spot(*shift) for shift in around] + [partner]
    peers += [at(*in_plane(*shift), z, core) for shift in plane]
    peers += [at(x, y, lax.rem(z + d, 8), core) for d in range(1, 8)]
    barrier = pltpu.get_barrier_semaphore()
    for peer in peers:
        pl.semaphore_signal(barrier, inc=1, device_id=peer, device_id_type=MESH)

    def remote(src, dst, sems, device):
        return pltpu.make_async_remote_copy(
            src_ref=src, dst_ref=dst, send_sem=sems.at[0], recv_sem=sems.at[1],
            device_id=device, device_id_type=MESH,
        )

    def put_row(field, row, value, mark=True):
        where = pl.ds(row * cols if isinstance(row, int) else pl.multiple_of(row * cols, cols), cols)
        field[where, mid] = value.astype(BF16)
        field[where, 0:ch] = pltpu.roll(value, 1, 0).astype(BF16)
        field[where, 2 * ch : 3 * ch] = pltpu.roll(value, cols - 1, 0).astype(BF16)
        if mark:
            edge[0, pl.ds(row - 1, 1), :] = value[0:1]
            edge[1, pl.ds(row - 1, 1), :] = value[cols - 1 : cols]

    def copies(index, field, which):
        if index == 0:
            first, last = in_ref.at[0], in_ref.at[rows - 1]
        else:
            first = field.at[cols : 2 * cols, mid]
            last = field.at[rows * cols : (rows + 1) * cols, mid]
        plan = [
            (first, field.at[(rows + 1) * cols : (rows + 2) * cols, mid], (-1, 0)),
            (last, field.at[0:cols, mid], (1, 0)),
        ]
        for dlat in (-1, 1, 0):
            plan.append((sent.at[index, 0], got.at[index, 1, 1 - dlat], (dlat, -1)))
            plan.append((sent.at[index, 1], got.at[index, 0, 1 - dlat], (dlat, 1)))
        return [
            pltpu.make_async_remote_copy(
                src_ref=plan[n][0], dst_ref=plan[n][1],
                send_sem=send_sem.at[index, n], recv_sem=recv_sem.at[index, n],
                device_id=spot(*plan[n][2]), device_id_type=MESH,
            )
            for n in which
        ]

    def send(index, field):
        for side in range(2):
            sent[index, side] = edge[side].astype(BF16)
        for copy in copies(index, field, range(8)):
            copy.start()

    up, down = lat > 0, lat < lats - 1

    def receive_sides(index, field):
        for copy in copies(index, field, (6, 7)):
            copy.wait()
        for side in range(2):
            halo[side, 8 : 8 + rows] = got[index, side, 1].astype(F32)
        spots = lax.broadcasted_iota(jnp.int32, (16, ch), 0)
        for row in range(1, rows + 1):
            head = slice(row * cols, row * cols + 16)
            tail = slice((row + 1) * cols - 16, (row + 1) * cols)
            left = halo[0, 7 + row : 8 + row, :]
            right = halo[1, 7 + row : 8 + row, :]
            field[head, 0:ch] = jnp.where(spots == 0, left, field[head, 0:ch].astype(F32)).astype(BF16)
            field[tail, 2 * ch : 3 * ch] = jnp.where(
                spots == 15, right, field[tail, 2 * ch : 3 * ch].astype(F32)
            ).astype(BF16)

    def receive_ends(index, field):
        for copy in copies(index, field, range(6)):
            copy.wait()
        place = lax.broadcasted_iota(jnp.int32, (cols, ch), 0)
        for row, valid, slot, pick in ((0, up, 0, rows - 1), (rows + 1, down, 2, 0)):
            where = slice(row * cols, (row + 1) * cols)
            value = jnp.where(valid, field[where, mid].astype(F32), 0.0)
            left, right = (
                jnp.where(valid, got[index, side, slot].astype(F32)[pick : pick + 1], 0.0)
                for side in range(2)
            )
            field[where, mid] = value.astype(BF16)
            field[where, 0:ch] = jnp.where(place == 0, left, pltpu.roll(value, 1, 0)).astype(BF16)
            field[where, 2 * ch : 3 * ch] = jnp.where(
                place == cols - 1, right, pltpu.roll(value, cols - 1, 0)
            ).astype(BF16)

    def conv(field, weight, start, count):
        total = None
        for a in range(3):
            piece = field[(start + a) * cols : (start + a + count) * cols, :]
            part = jnp.dot(piece, weight[a], preferred_element_type=F32)
            total = part if total is None else total + part
        return total

    def conv_t(field, weight, start, count):
        total = None
        for a in range(3):
            for b in range(3):
                piece = field[(start + a) * cols : (start + a + count) * cols, b * ch : (b + 1) * ch]
                part = lax.dot_general(
                    piece, weight[2 - a, (2 - b) * ch : (3 - b) * ch, :],
                    (((1,), (1,)), ((), ())), preferred_element_type=F32,
                )
                total = part if total is None else total + part
        return total

    def put_rows(field, start, count, value):
        for k in range(count):
            put_row(field, start + 1 + k, value[k * cols : (k + 1) * cols])

    def middle(step):
        for start in range(group, rows - group, MID):
            step(start, MID)

    def outer(step):
        step(0, group)
        step(rows - group, group)

    own_rows = pl.ds(pl.multiple_of(core * half, half), half)
    other_rows = pl.ds(pl.multiple_of((1 - core) * half, half), half)

    def chunk(px, py):
        return pl.ds(pl.multiple_of((px * 4 + py) * 16, 16), 16)

    my_chunk = chunk(x, y)

    pieces = [(0, 3 * a, 3) for a in range(3)] + [(1, t, 1) for t in range(9)]
    number = {piece: n for n, piece in enumerate(pieces)}

    def taps(piece):
        return slice(piece[1], piece[1] + piece[2])

    def lanes(piece):
        first = piece[1] % 3
        return slice(first * ch, (first + piece[2]) * ch)

    def pair_copy(piece):
        g, t, _ = piece
        return remote(
            grads.at[g, t // 3, other_rows, lanes(piece)], pair.at[g, t // 3, :, lanes(piece)],
            pair_sem.at[number[piece]], partner,
        )

    def settle(ref, sems):
        pltpu.make_async_copy(ref, ref, sems.at[0]).wait()
        pltpu.make_async_copy(ref, ref, sems.at[1]).wait()

    def grad_piece(g, a, field):
        grads[g, a] = jnp.dot(
            turned[...], field[a * cols : (a + rows) * cols, :], preferred_element_type=F32
        )
        for piece in pieces:
            if piece[0] == g and piece[1] // 3 == a:
                pair_copy(piece).start()

    def scatter(piece):
        g, first, count = piece
        pair_copy(piece).wait()
        for t in range(first, first + count):
            a, b = t // 3, t % 3
            where = slice(b * ch, (b + 1) * ch)
            total = (grads[g, a, own_rows, where] + pair[g, a, :, where]).T
            mine[g, t] = total
            out1[g, t] = total.astype(BF16)
        for n, shift in enumerate(plane):
            px, py = in_plane(*shift)
            remote(
                out1.at[g, taps(piece), chunk(px, py), :], in1.at[g, taps(piece), n],
                plane_sem.at[number[piece]], at(px, py, z, core),
            ).start()

    def depth(piece):
        g = piece[0]
        settle(in1.at[g, taps(piece)], plane_sem.at[number[piece]])
        total = mine[g, taps(piece), my_chunk, :]
        for n in range(15):
            total = total + in1[g, taps(piece), n].astype(F32)
        zin[g, taps(piece), z] = total.astype(BF16)
        for d in range(1, 8):
            place = zin.at[g, taps(piece), z]
            remote(place, place, z_sem.at[number[piece]], at(x, y, lax.rem(z + d, 8), core)).start()

    def spread(piece):
        g = piece[0]
        settle(zin.at[g, taps(piece), 0:7], z_sem.at[number[piece]])
        total = zin[g, taps(piece), 0].astype(F32)
        for n in range(1, 8):
            total = total + zin[g, taps(piece), n].astype(F32)
        final[g, core, taps(piece), my_chunk, :] = total.astype(BF16)
        place = final.at[g, core, taps(piece), my_chunk, :]
        for shift in plane:
            px, py = in_plane(*shift)
            remote(place, place, spread_sem.at[number[piece]], at(px, py, z, core)).start()

    def last_copy(piece):
        place = final.at[piece[0], core, taps(piece)]
        return remote(place, place, last_sem.at[number[piece]], partner)

    def join(piece):
        settle(in1.at[piece[0], taps(piece)], spread_sem.at[number[piece]])
        last_copy(piece).start()

    def finish(piece):
        last_copy(piece).wait()
        out = (o2_ref, o1_ref)[piece[0]]
        for c in range(2):
            out[taps(piece), :, c * half : (c + 1) * half] = final[piece[0], c, taps(piece)]

    early, late = pieces[:3], [pieces[3 + 3 * a : 6 + 3 * a] for a in range(3)]

    def each(step, some):
        for piece in some:
            step(piece)

    loads[0].wait()
    for row in range(rows):
        edge[0, row : row + 1] = in_ref[row, 0:16].astype(F32)[0:1]
        edge[1, row : row + 1] = in_ref[row, cols - 16 : cols].astype(F32)[15:16]
    pl.semaphore_wait(barrier, len(peers))
    send(0, xs)

    def load(row, carry):
        put_row(xs, row + 1, in_ref[row].astype(F32), mark=False)
        return carry

    lax.fori_loop(0, rows, load, 0)
    loads[1].wait()

    def span(start, count):
        return slice(start * cols, (start + count) * cols)

    def first(start, count):
        value = conv(xs, w1_ref, start, count)
        part, slope = slope_parts(value)
        slope1[span(start, count), :] = slope
        put_rows(acts, start, count, value * part)

    receive_sides(0, xs)
    middle(first)
    receive_ends(0, xs)
    outer(first)
    send(1, acts)
    loads[2].wait()
    loads[3].wait()

    def second(start, count):
        value = conv(acts, w2_ref, start, count)
        _, slope = slope_parts(value)
        rate = cot_ref[start : start + count].astype(F32).reshape(count * cols, ch)
        delta = rate * slope
        put_rows(d2s, start, count, delta)
        turned[:, span(start, count)] = delta.T.astype(BF16)

    receive_sides(1, acts)
    middle(second)
    receive_ends(1, acts)
    outer(second)
    send(2, d2s)
    grad_piece(0, 0, acts)
    grad_piece(0, 1, acts)
    scatter(early[0])
    grad_piece(0, 2, acts)

    def third(start, count):
        value = conv_t(d2s, w2_ref, start, count)
        delta = value * slope1[span(start, count), :]
        put_rows(d1s, start, count, delta)
        turned[:, span(start, count)] = delta.T.astype(BF16)

    receive_sides(2, d2s)
    middle(third)
    each(scatter, early[1:])
    receive_ends(2, d2s)
    outer(third)
    send(3, d1s)
    grad_piece(1, 0, xs)
    grad_piece(1, 1, xs)
    each(scatter, late[0])
    depth(early[0])
    grad_piece(1, 2, xs)
    each(scatter, late[1])

    def fourth(start, count):
        value = conv_t(d1s, w1_ref, start, count)
        dx_ref[start : start + count] = value.astype(BF16).reshape(count, cols, ch)

    receive_sides(3, d1s)
    middle(fourth)
    each(scatter, late[2])
    depth(early[1])
    receive_ends(3, d1s)
    outer(fourth)
    depth(early[2])
    each(depth, late[0])
    spread(early[0])
    each(depth, late[1])
    spread(early[1])
    each(depth, late[2])
    spread(early[2])
    each(spread, late[0])
    join(early[0])
    each(spread, late[1])
    join(early[1])
    each(spread, late[2])
    join(early[2])
    each(finish, early)
    for some in late:
        each(join, some)
    for some in late:
        each(finish, some)


def write_kernel(dx_ref, g1_ref, g2_ref, dx_out, o1_out, o2_out, wide, sems):
    copies = [pltpu.make_async_copy(dx_ref, dx_out, sems.at[18])]
    copies[0].start()
    for n, (ref, out) in enumerate(((g1_ref, o1_out), (g2_ref, o2_out))):
        for t in range(9):
            wide[n, t] = ref[t].astype(F32)
            copies.append(pltpu.make_async_copy(wide.at[n, t], out.at[t], sems.at[9 * n + t]))
            copies[-1].start()
    for copy in copies:
        copy.wait()


def body(lats, lons, inputs, first_filter, second_filter, cotangent):
    rows, cols, ch = inputs.shape
    group = 4
    vmem = pl.BlockSpec(memory_space=pltpu.VMEM)
    hbm = pl.BlockSpec(memory_space=pltpu.HBM)
    cells = rows * cols
    half = ch // 2
    padded = pltpu.VMEM(((rows + 2) * cols, 3 * ch), BF16)
    dma = pltpu.SemaphoreType.DMA
    dx, o1, o2 = pl.pallas_call(
        functools.partial(kernel, lats, lons, rows, cols, ch, group),
        out_shape=(
            jax.ShapeDtypeStruct((rows, cols, ch), BF16),
            jax.ShapeDtypeStruct((9, ch, ch), BF16),
            jax.ShapeDtypeStruct((9, ch, ch), BF16),
        ),
        in_specs=[hbm] * 4,
        out_specs=(vmem,) * 3,
        scratch_shapes=[
            pltpu.VMEM((rows, cols, ch), BF16),
            pltpu.VMEM((3, 3 * ch, ch), BF16),
            pltpu.VMEM((3, 3 * ch, ch), BF16),
            pltpu.VMEM((rows, cols, ch), BF16),
            padded, padded, padded, padded,
            pltpu.VMEM((cells, ch), F32),
            pltpu.VMEM((ch, cells), BF16),
            pltpu.VMEM((2, rows, ch), F32),
            pltpu.VMEM((4, 2, rows, ch), BF16),
            pltpu.VMEM((4, 2, 3, rows, ch), BF16),
            pltpu.VMEM((2, 16 + rows, ch), F32),
            pltpu.VMEM((2, 3, ch, 3 * ch), F32),
            pltpu.VMEM((2, 3, half, 3 * ch), F32),
            pltpu.VMEM((2, 9, ch, half), F32),
            pltpu.VMEM((2, 9, ch, half), BF16),
            pltpu.VMEM((2, 9, 15, 16, half), BF16),
            pltpu.VMEM((2, 9, 8, 16, half), BF16),
            pltpu.VMEM((2, 2, 9, ch, half), BF16),
            dma((4,)), dma((4, 8)), dma((4, 8)),
            dma((12, 2)), dma((12, 2)), dma((12, 2)), dma((12, 2)), dma((12, 2)),
        ],
        compiler_params=pltpu.CompilerParams(
            collective_id=0, has_side_effects=True, vmem_limit_bytes=VMEM_LIMIT
        ),
        name="stages",
    )(
        *(
            pltpu.with_memory_space_constraint(value, pltpu.HBM)
            for value in (
                inputs,
                first_filter.reshape(3, 3 * ch, ch),
                second_filter.reshape(3, 3 * ch, ch),
                cotangent,
            )
        )
    )
    dx, o1, o2 = pl.pallas_call(
        write_kernel,
        out_shape=(
            jax.ShapeDtypeStruct((rows, cols, ch), BF16),
            jax.ShapeDtypeStruct((9, ch, ch), F32),
            jax.ShapeDtypeStruct((9, ch, ch), F32),
        ),
        in_specs=[vmem] * 3,
        out_specs=(hbm,) * 3,
        scratch_shapes=[pltpu.VMEM((2, 9, ch, ch), F32), dma((19,))],
        compiler_params=pltpu.CompilerParams(vmem_limit_bytes=12 * 1024 * 1024),
        name="write",
    )(dx, o1, o2)
    return dx, o1.reshape(3, 3, ch, ch), o2.reshape(3, 3, ch, ch)


def solution(mesh):
    in_specs = (P("lat", "lon", None), P(), P(), P("lat", "lon", None))
    out_specs = (P("lat", "lon", None), P(), P())
    step = functools.partial(body, mesh.shape["lat"], mesh.shape["lon"])
    return jax.shard_map(step, mesh=mesh, in_specs=in_specs, out_specs=out_specs, check_vma=False)
```

```python
import functools

import jax
import jax.numpy as jnp
from jax import lax
from jax.experimental import pallas as pl
from jax.experimental.pallas import tpu as pltpu
from jax.sharding import PartitionSpec as P

MESH = pl.DeviceIdType.MESH
F32 = jnp.float32
BF16 = jnp.bfloat16
VMEM_LIMIT = 48 * 1024 * 1024
B1, B2, B3, B4 = 4, 4, 4, 4


def half_erf(value):
    return 0.5 * (1.0 + lax.erf(value * 0.7071067811865476))


def slope_of(value):
    return half_erf(value) + value * jnp.exp(-0.5 * value * value) * 0.3989422804014327


def kernel(
    lats, lons, rows, cols, ch, group,
    in_hbm, w1_hbm, w2_hbm, cot_hbm,
    dx_ref, final, o2_ref,
    in_ref, w1_ref, w2_ref, cot_ref, wt1, wt2,
    xs, acts, d2s, d1s, partial, slope1, turned, edge, sent, got, halo,
    grads, pair, mine, out1, in1, zin,
    load_sem, send_sem, recv_sem,
    pair_sem, plane_sem, z_sem, spread_sem, last_sem,
):
    lat, lon = lax.axis_index("lat"), lax.axis_index("lon")
    core = lax.rem(lat, 2)
    x = lax.rem(lat // 2, 2) * 2 + lon // 8
    y = lat // 4
    z = lax.rem(lon, 8)
    size = group * cols
    half = ch // 2
    mid = slice(ch, 2 * ch)

    loads = [
        pltpu.make_async_copy(src, dst, load_sem.at[n])
        for n, (src, dst) in enumerate(
            ((in_hbm, in_ref), (w1_hbm, w1_ref), (cot_hbm, cot_ref), (w2_hbm, w2_ref))
        )
    ]
    for copy in loads:
        copy.start()

    def spot(dlat, dlon):
        return {"lat": lax.rem(lat + dlat + lats, lats), "lon": lax.rem(lon + dlon + lons, lons)}

    def at(x, y, z, core):
        return {"lat": y * 4 + (x // 2) * 2 + core, "lon": lax.rem(x, 2) * 8 + z}

    partner = at(x, y, z, 1 - core)
    plane = [(dx, dy) for dx in range(4) for dy in range(4) if dx or dy]

    def in_plane(dx, dy):
        return lax.rem(x + dx, 4), lax.rem(y + dy, 4)

    around = [(dlat, dlon) for dlat in (-1, 0, 1) for dlon in (-1, 0, 1) if dlat or dlon]
    peers = [spot(*shift) for shift in around] + [partner]
    peers += [at(*in_plane(*shift), z, core) for shift in plane]
    peers += [at(x, y, lax.rem(z + d, 8), core) for d in range(1, 8)]
    barrier = pltpu.get_barrier_semaphore()
    for peer in peers:
        pl.semaphore_signal(barrier, inc=1, device_id=peer, device_id_type=MESH)

    def remote(src, dst, sems, device):
        return pltpu.make_async_remote_copy(
            src_ref=src, dst_ref=dst, send_sem=sems.at[0], recv_sem=sems.at[1],
            device_id=device, device_id_type=MESH,
        )

    def line(row):
        return pl.ds(row * cols if isinstance(row, int) else pl.multiple_of(row * cols, cols), cols)

    def put_mid(field, row, value, mark=True):
        field[line(row), mid] = value.astype(BF16)
        if mark:
            edge[0, row - 1 : row] = value[0:1]
            edge[1, row - 1 : row] = value[cols - 1 : cols]

    def put_sides(field, row, value):
        field[line(row), 0:ch] = pltpu.roll(value, 1, 0).astype(BF16)
        field[line(row), 2 * ch : 3 * ch] = pltpu.roll(value, cols - 1, 0).astype(BF16)

    def copies(index, field, which):
        if index == 0:
            first, last = in_ref.at[0], in_ref.at[rows - 1]
        else:
            first = field.at[cols : 2 * cols, mid]
            last = field.at[rows * cols : (rows + 1) * cols, mid]
        plan = [
            (first, field.at[(rows + 1) * cols : (rows + 2) * cols, mid], (-1, 0)),
            (last, field.at[0:cols, mid], (1, 0)),
        ]
        for dlat in (-1, 1, 0):
            plan.append((sent.at[index, 0], got.at[index, 1, 1 - dlat], (dlat, -1)))
            plan.append((sent.at[index, 1], got.at[index, 0, 1 - dlat], (dlat, 1)))
        return [
            pltpu.make_async_remote_copy(
                src_ref=plan[n][0], dst_ref=plan[n][1],
                send_sem=send_sem.at[index, n], recv_sem=recv_sem.at[index, n],
                device_id=spot(*plan[n][2]), device_id_type=MESH,
            )
            for n in which
        ]

    def send(index, field):
        for side in range(2):
            sent[index, side] = edge[side].astype(BF16)
        for copy in copies(index, field, range(8)):
            copy.start()

    up, down = lat > 0, lat < lats - 1

    def receive_sides(index, field):
        for copy in copies(index, field, (6, 7)):
            copy.wait()
        for side in range(2):
            halo[side, 8 : 8 + rows] = got[index, side, 1].astype(F32)
        spots = lax.broadcasted_iota(jnp.int32, (16, ch), 0)
        for row in range(1, rows + 1):
            head = slice(row * cols, row * cols + 16)
            tail = slice((row + 1) * cols - 16, (row + 1) * cols)
            left = halo[0, 7 + row : 8 + row, :]
            right = halo[1, 7 + row : 8 + row, :]
            field[head, 0:ch] = jnp.where(spots == 0, left, field[head, 0:ch].astype(F32)).astype(BF16)
            field[tail, 2 * ch : 3 * ch] = jnp.where(
                spots == 15, right, field[tail, 2 * ch : 3 * ch].astype(F32)
            ).astype(BF16)

    def receive_ends(index, field):
        for copy in copies(index, field, range(6)):
            copy.wait()
        place = lax.broadcasted_iota(jnp.int32, (cols, ch), 0)
        for row, valid, slot, pick in ((0, up, 0, rows - 1), (rows + 1, down, 2, 0)):
            where = slice(row * cols, (row + 1) * cols)
            value = jnp.where(valid, field[where, mid].astype(F32), 0.0)
            left, right = (
                jnp.where(valid, got[index, side, slot].astype(F32)[pick : pick + 1], 0.0)
                for side in range(2)
            )
            field[where, mid] = value.astype(BF16)
            field[where, 0:ch] = jnp.where(place == 0, left, pltpu.roll(value, 1, 0)).astype(BF16)
            field[where, 2 * ch : 3 * ch] = jnp.where(
                place == cols - 1, right, pltpu.roll(value, cols - 1, 0)
            ).astype(BF16)

    def conv(field, weight, start, count):
        total = None
        for a in range(3):
            piece = field[(start + a) * cols : (start + a + count) * cols, :]
            part = jnp.dot(piece, weight[a], preferred_element_type=F32)
            total = part if total is None else total + part
        return total

    def flip(source, target):
        for a in range(3):
            for b in range(3):
                target[a, b * ch : (b + 1) * ch, :] = source[2 - a, (2 - b) * ch : (3 - b) * ch, :].T

    def centre(field, weight, start, count, steps):
        total = None
        for a in steps:
            piece = field[(start + a) * cols : (start + a + count) * cols, mid]
            part = jnp.dot(piece, weight[a, mid, :], preferred_element_type=F32)
            total = part if total is None else total + part
        partial[start * cols : (start + count) * cols, :] = total

    def centres(field, weight):
        for start in range(0, rows, group):
            steps = (1, 2) if start == 0 else (0, 1) if start == rows - group else (0, 1, 2)
            centre(field, weight, start, group, steps)

    def conv_rest(field, weight, start, count):
        total = partial[start * cols : (start + count) * cols, :]
        for a in range(3):
            where = slice((start + a) * cols, (start + a + count) * cols)
            for b in (0, 2):
                lanes_b = slice(b * ch, (b + 1) * ch)
                total = total + jnp.dot(
                    field[where, lanes_b], weight[a, lanes_b, :], preferred_element_type=F32
                )
        if start in (0, rows - group):
            a = 0 if start == 0 else 2
            where = slice((start + a) * cols, (start + a + count) * cols)
            total = total + jnp.dot(field[where, mid], weight[a, mid, :], preferred_element_type=F32)
        return total

    def put_rows(field, start, count, value, sides):
        for k in range(count):
            part = value[k * cols : (k + 1) * cols]
            put_mid(field, start + 1 + k, part)
            if sides:
                put_sides(field, start + 1 + k, part)

    def middle(step, block):
        for start in range(group, rows - group, block):
            step(start, block)

    def outer(step, block):
        for base in (0, rows - group):
            for start in range(base, base + group, block):
                step(start, block)

    own_rows = pl.ds(pl.multiple_of(core * half, half), half)
    other_rows = pl.ds(pl.multiple_of((1 - core) * half, half), half)

    def chunk(px, py):
        return pl.ds(pl.multiple_of((px * 4 + py) * 16, 16), 16)

    my_chunk = chunk(x, y)

    pieces = [(0, 3 * a, 3) for a in range(3)] + [(1, t, 1) for t in range(9)]
    number = {piece: n for n, piece in enumerate(pieces)}

    def taps(piece):
        return slice(piece[1], piece[1] + piece[2])

    def lanes(piece):
        first = piece[1] % 3
        return slice(first * ch, (first + piece[2]) * ch)

    def pair_copy(piece):
        g, t, _ = piece
        return remote(
            grads.at[g, t // 3, other_rows, lanes(piece)], pair.at[g, t // 3, :, lanes(piece)],
            pair_sem.at[number[piece]], partner,
        )

    def settle(ref, sems):
        pltpu.make_async_copy(ref, ref, sems.at[0]).wait()
        pltpu.make_async_copy(ref, ref, sems.at[1]).wait()

    def grad_piece(g, a, field):
        grads[g, a] = jnp.dot(
            turned[...], field[a * cols : (a + rows) * cols, :], preferred_element_type=F32
        )
        for piece in pieces:
            if piece[0] == g and piece[1] // 3 == a:
                pair_copy(piece).start()

    def scatter(piece):
        g, first, count = piece
        pair_copy(piece).wait()
        for t in range(first, first + count):
            a, b = t // 3, t % 3
            where = slice(b * ch, (b + 1) * ch)
            total = (grads[g, a, own_rows, where] + pair[g, a, :, where]).T
            mine[g, t] = total
            out1[g, t] = total.astype(BF16)
        for n, shift in enumerate(plane):
            px, py = in_plane(*shift)
            remote(
                out1.at[g, taps(piece), chunk(px, py), :], in1.at[g, taps(piece), n],
                plane_sem.at[number[piece]], at(px, py, z, core),
            ).start()

    def depth(piece):
        g = piece[0]
        settle(in1.at[g, taps(piece)], plane_sem.at[number[piece]])
        total = mine[g, taps(piece), my_chunk, :]
        for n in range(15):
            total = total + in1[g, taps(piece), n].astype(F32)
        zin[g, taps(piece), z] = total.astype(BF16)
        for d in range(1, 8):
            place = zin.at[g, taps(piece), z]
            remote(place, place, z_sem.at[number[piece]], at(x, y, lax.rem(z + d, 8), core)).start()

    def spread(piece):
        g = piece[0]
        settle(zin.at[g, taps(piece), 0:7], z_sem.at[number[piece]])
        total = zin[g, taps(piece), 0].astype(F32)
        for n in range(1, 8):
            total = total + zin[g, taps(piece), n].astype(F32)
        final[g, core, taps(piece), my_chunk, :] = total.astype(BF16)
        place = final.at[g, core, taps(piece), my_chunk, :]
        for shift in plane:
            px, py = in_plane(*shift)
            remote(place, place, spread_sem.at[number[piece]], at(px, py, z, core)).start()

    def last_copy(piece):
        place = final.at[piece[0], core, taps(piece)]
        return remote(place, place, last_sem.at[number[piece]], partner)

    def join(piece):
        settle(in1.at[piece[0], taps(piece)], spread_sem.at[number[piece]])
        last_copy(piece).start()

    def finish(piece):
        last_copy(piece).wait()
        if piece[0] == 0:
            for c in range(2):
                o2_ref[taps(piece), :, c * half : (c + 1) * half] = final[0, c, taps(piece)].astype(F32)

    early, late = pieces[:3], pieces[3:]

    def each(step, some):
        for piece in some:
            step(piece)

    loads[0].wait()
    for row in range(rows):
        edge[0, row : row + 1] = in_ref[row, 0:16].astype(F32)[0:1]
        edge[1, row : row + 1] = in_ref[row, cols - 16 : cols].astype(F32)[15:16]
    pl.semaphore_wait(barrier, len(peers))
    send(0, xs)

    def load(row, carry):
        value = in_ref[row].astype(F32)
        put_mid(xs, row + 1, value, mark=False)
        put_sides(xs, row + 1, value)
        return carry

    lax.fori_loop(0, rows, load, 0)
    for copy in loads[1:]:
        copy.wait()
    flip(w1_ref, wt1)
    flip(w2_ref, wt2)

    def span(start, count):
        return slice(start * cols, (start + count) * cols)

    def first(start, count):
        value = conv_rest(xs, w1_ref, start, count)
        slope1[span(start, count), :] = value
        put_rows(acts, start, count, value * half_erf(value), False)

    centres(xs, w1_ref)
    receive_sides(0, xs)
    middle(first, B1)
    receive_ends(0, xs)
    outer(first, B1)
    send(1, acts)

    def fill(row, carry):
        where = pl.ds(pl.multiple_of(row * cols, cols), cols)
        slope1[where, :] = slope_of(slope1[where, :])
        put_sides(acts, row + 1, acts[line(row + 1), mid].astype(F32))
        return carry

    lax.fori_loop(0, rows, fill, 0)

    def second(start, count):
        value = conv_rest(acts, w2_ref, start, count)
        rate = cot_ref[start : start + count].astype(F32).reshape(count * cols, ch)
        delta = rate * slope_of(value)
        put_rows(d2s, start, count, delta, True)
        turned[:, span(start, count)] = delta.astype(BF16).T

    centres(acts, w2_ref)
    receive_sides(1, acts)
    middle(second, B2)
    receive_ends(1, acts)
    outer(second, B2)
    send(2, d2s)
    grad_piece(0, 0, acts)
    grad_piece(0, 1, acts)
    grad_piece(0, 2, acts)
    scatter(early[0])

    def third(start, count):
        value = conv(d2s, wt2, start, count)
        delta = value * slope1[span(start, count), :]
        put_rows(d1s, start, count, delta, False)
        turned[:, span(start, count)] = delta.astype(BF16).T

    receive_sides(2, d2s)
    middle(third, B3)
    scatter(early[1])
    scatter(early[2])
    receive_ends(2, d2s)
    outer(third, B3)
    send(3, d1s)
    grad_piece(1, 0, xs)
    grad_piece(1, 1, xs)
    each(scatter, late[:3])
    depth(early[0])
    grad_piece(1, 2, xs)
    each(scatter, late[3:6])
    depth(early[1])
    each(scatter, late[6:])
    for row in range(1, rows + 1):
        put_sides(d1s, row, d1s[line(row), mid].astype(F32))

    def fourth(start, count):
        value = conv(d1s, wt1, start, count)
        dx_ref[start : start + count] = value.astype(BF16).reshape(count, cols, ch)

    receive_sides(3, d1s)
    depth(early[2])
    middle(fourth, B4)
    receive_ends(3, d1s)
    outer(fourth, B4)
    each(depth, late[:3])
    spread(early[0])
    each(depth, late[3:6])
    spread(early[1])
    each(depth, late[6:])
    spread(early[2])
    each(spread, late)
    each(join, early)
    each(join, late[:3])
    each(finish, early)
    each(join, late[3:])
    each(finish, late)


def write_kernel(dx_ref, final, g2_ref, dx_out, o1_out, o2_out, wide, sems):
    half = final.shape[-1]
    copies = [
        pltpu.make_async_copy(g2_ref, o2_out, sems.at[9]),
        pltpu.make_async_copy(dx_ref, dx_out, sems.at[10]),
    ]
    for copy in copies:
        copy.start()
    for t in range(9):
        for c in range(2):
            wide[t, :, c * half : (c + 1) * half] = final[1, c, t].astype(F32)
        copies.append(pltpu.make_async_copy(wide.at[t], o1_out.at[t], sems.at[t]))
        copies[-1].start()
    for copy in copies:
        copy.wait()


def body(lats, lons, inputs, first_filter, second_filter, cotangent):
    rows, cols, ch = inputs.shape
    group = 4
    vmem = pl.BlockSpec(memory_space=pltpu.VMEM)
    hbm = pl.BlockSpec(memory_space=pltpu.HBM)
    cells = rows * cols
    half = ch // 2
    padded = pltpu.VMEM(((rows + 2) * cols, 3 * ch), BF16)
    dma = pltpu.SemaphoreType.DMA
    dx, final, o2 = pl.pallas_call(
        functools.partial(kernel, lats, lons, rows, cols, ch, group),
        out_shape=(
            jax.ShapeDtypeStruct((rows, cols, ch), BF16),
            jax.ShapeDtypeStruct((2, 2, 9, ch, half), BF16),
            jax.ShapeDtypeStruct((9, ch, ch), F32),
        ),
        in_specs=[hbm] * 4,
        out_specs=(vmem,) * 3,
        scratch_shapes=[
            pltpu.VMEM((rows, cols, ch), BF16),
            pltpu.VMEM((3, 3 * ch, ch), BF16),
            pltpu.VMEM((3, 3 * ch, ch), BF16),
            pltpu.VMEM((rows, cols, ch), BF16),
            pltpu.VMEM((3, 3 * ch, ch), BF16),
            pltpu.VMEM((3, 3 * ch, ch), BF16),
            padded, padded, padded, padded,
            pltpu.VMEM((cells, ch), F32),
            pltpu.VMEM((cells, ch), F32),
            pltpu.VMEM((ch, cells), BF16),
            pltpu.VMEM((2, rows, ch), F32),
            pltpu.VMEM((4, 2, rows, ch), BF16),
            pltpu.VMEM((4, 2, 3, rows, ch), BF16),
            pltpu.VMEM((2, 16 + rows, ch), F32),
            pltpu.VMEM((2, 3, ch, 3 * ch), F32),
            pltpu.VMEM((2, 3, half, 3 * ch), F32),
            pltpu.VMEM((2, 9, ch, half), F32),
            pltpu.VMEM((2, 9, ch, half), BF16),
            pltpu.VMEM((2, 9, 15, 16, half), BF16),
            pltpu.VMEM((2, 9, 8, 16, half), BF16),
            dma((4,)), dma((4, 8)), dma((4, 8)),
            dma((12, 2)), dma((12, 2)), dma((12, 2)), dma((12, 2)), dma((12, 2)),
        ],
        compiler_params=pltpu.CompilerParams(
            collective_id=0, has_side_effects=True, vmem_limit_bytes=VMEM_LIMIT
        ),
        name="stages",
    )(
        *(
            pltpu.with_memory_space_constraint(value, pltpu.HBM)
            for value in (
                inputs,
                first_filter.reshape(3, 3 * ch, ch),
                second_filter.reshape(3, 3 * ch, ch),
                cotangent,
            )
        )
    )
    dx, o1, o2 = pl.pallas_call(
        write_kernel,
        out_shape=(
            jax.ShapeDtypeStruct((rows, cols, ch), BF16),
            jax.ShapeDtypeStruct((9, ch, ch), F32),
            jax.ShapeDtypeStruct((9, ch, ch), F32),
        ),
        in_specs=[vmem] * 3,
        out_specs=(hbm,) * 3,
        scratch_shapes=[pltpu.VMEM((9, ch, ch), F32), dma((11,))],
        compiler_params=pltpu.CompilerParams(vmem_limit_bytes=12 * 1024 * 1024),
        name="write",
    )(dx, final, o2)
    return dx, o1.reshape(3, 3, ch, ch), o2.reshape(3, 3, ch, ch)


def solution(mesh):
    in_specs = (P("lat", "lon", None), P(), P(), P("lat", "lon", None))
    out_specs = (P("lat", "lon", None), P(), P())
    step = functools.partial(body, mesh.shape["lat"], mesh.shape["lon"])
    return jax.shard_map(step, mesh=mesh, in_specs=in_specs, out_specs=out_specs, check_vma=False)
```

```python
import functools

import jax
import jax.numpy as jnp
from jax import lax
from jax.experimental import pallas as pl
from jax.experimental.pallas import tpu as pltpu
from jax.sharding import PartitionSpec as P

MESH = pl.DeviceIdType.MESH
F32 = jnp.float32
BF16 = jnp.bfloat16
VMEM_LIMIT = 48 * 1024 * 1024
B1, B2, B3, B4 = 4, 4, 4, 4


def half_erf(value):
    return 0.5 * (1.0 + lax.erf(value * 0.7071067811865476))


def slope_of(value):
    return half_erf(value) + value * jnp.exp(-0.5 * value * value) * 0.3989422804014327


def kernel(
    lats, lons, rows, cols, ch, group,
    in_hbm, w1_hbm, w2_hbm, cot_hbm,
    dx_ref, final, o2_ref,
    in_ref, w1_ref, w2_ref, cot_ref, wt1, wt2,
    xs, acts, d2s, d1s, partial, slope1, turned, edge, sent, got, halo,
    grads, pair, mine, out1, in1, zin,
    load_sem, send_sem, recv_sem,
    pair_sem, plane_sem, z_sem, spread_sem, last_sem,
):
    lat, lon = lax.axis_index("lat"), lax.axis_index("lon")
    core = lax.rem(lat, 2)
    x = lax.rem(lat // 2, 2) * 2 + lon // 8
    y = lat // 4
    z = lax.rem(lon, 8)
    size = group * cols
    half = ch // 2
    mid = slice(ch, 2 * ch)

    loads = [
        pltpu.make_async_copy(src, dst, load_sem.at[n])
        for n, (src, dst) in enumerate(
            ((in_hbm, in_ref), (w1_hbm, w1_ref), (cot_hbm, cot_ref), (w2_hbm, w2_ref))
        )
    ]
    for copy in loads:
        copy.start()

    def spot(dlat, dlon):
        return {"lat": lax.rem(lat + dlat + lats, lats), "lon": lax.rem(lon + dlon + lons, lons)}

    def at(x, y, z, core):
        return {"lat": y * 4 + (x // 2) * 2 + core, "lon": lax.rem(x, 2) * 8 + z}

    partner = at(x, y, z, 1 - core)
    plane = [(dx, dy) for dx in range(4) for dy in range(4) if dx or dy]

    def in_plane(dx, dy):
        return lax.rem(x + dx, 4), lax.rem(y + dy, 4)

    around = [(dlat, dlon) for dlat in (-1, 0, 1) for dlon in (-1, 0, 1) if dlat or dlon]
    peers = [spot(*shift) for shift in around] + [partner]
    peers += [at(*in_plane(*shift), z, core) for shift in plane]
    peers += [at(x, y, lax.rem(z + d, 8), core) for d in range(1, 8)]
    barrier = pltpu.get_barrier_semaphore()
    for peer in peers:
        pl.semaphore_signal(barrier, inc=1, device_id=peer, device_id_type=MESH)

    def remote(src, dst, sems, device):
        return pltpu.make_async_remote_copy(
            src_ref=src, dst_ref=dst, send_sem=sems.at[0], recv_sem=sems.at[1],
            device_id=device, device_id_type=MESH,
        )

    def line(row):
        return pl.ds(row * cols if isinstance(row, int) else pl.multiple_of(row * cols, cols), cols)

    def put_mid(field, row, value, mark=True):
        field[line(row), mid] = value.astype(BF16)
        if mark:
            edge[0, row - 1 : row] = value[0:1]
            edge[1, row - 1 : row] = value[cols - 1 : cols]

    def put_sides(field, row, value):
        field[line(row), 0:ch] = pltpu.roll(value, 1, 0).astype(BF16)
        field[line(row), 2 * ch : 3 * ch] = pltpu.roll(value, cols - 1, 0).astype(BF16)

    def copies(index, field, which):
        if index == 0:
            first, last = in_ref.at[0], in_ref.at[rows - 1]
        else:
            first = field.at[cols : 2 * cols, mid]
            last = field.at[rows * cols : (rows + 1) * cols, mid]
        plan = [
            (first, field.at[(rows + 1) * cols : (rows + 2) * cols, mid], (-1, 0)),
            (last, field.at[0:cols, mid], (1, 0)),
        ]
        for dlat in (-1, 1, 0):
            plan.append((sent.at[index, 0], got.at[index, 1, 1 - dlat], (dlat, -1)))
            plan.append((sent.at[index, 1], got.at[index, 0, 1 - dlat], (dlat, 1)))
        return [
            pltpu.make_async_remote_copy(
                src_ref=plan[n][0], dst_ref=plan[n][1],
                send_sem=send_sem.at[index, n], recv_sem=recv_sem.at[index, n],
                device_id=spot(*plan[n][2]), device_id_type=MESH,
            )
            for n in which
        ]

    def send(index, field):
        for side in range(2):
            sent[index, side] = edge[side].astype(BF16)
        for copy in copies(index, field, range(8)):
            copy.start()

    up, down = lat > 0, lat < lats - 1

    def receive_sides(index, field):
        for copy in copies(index, field, (6, 7)):
            copy.wait()
        for side in range(2):
            halo[side, 8 : 8 + rows] = got[index, side, 1].astype(F32)
        spots = lax.broadcasted_iota(jnp.int32, (16, ch), 0)
        for row in range(1, rows + 1):
            head = slice(row * cols, row * cols + 16)
            tail = slice((row + 1) * cols - 16, (row + 1) * cols)
            left = halo[0, 7 + row : 8 + row, :]
            right = halo[1, 7 + row : 8 + row, :]
            field[head, 0:ch] = jnp.where(spots == 0, left, field[head, 0:ch].astype(F32)).astype(BF16)
            field[tail, 2 * ch : 3 * ch] = jnp.where(
                spots == 15, right, field[tail, 2 * ch : 3 * ch].astype(F32)
            ).astype(BF16)

    def receive_ends(index, field):
        for copy in copies(index, field, range(6)):
            copy.wait()
        place = lax.broadcasted_iota(jnp.int32, (cols, ch), 0)
        for row, valid, slot, pick in ((0, up, 0, rows - 1), (rows + 1, down, 2, 0)):
            where = slice(row * cols, (row + 1) * cols)
            value = jnp.where(valid, field[where, mid].astype(F32), 0.0)
            left, right = (
                jnp.where(valid, got[index, side, slot].astype(F32)[pick : pick + 1], 0.0)
                for side in range(2)
            )
            field[where, mid] = value.astype(BF16)
            field[where, 0:ch] = jnp.where(place == 0, left, pltpu.roll(value, 1, 0)).astype(BF16)
            field[where, 2 * ch : 3 * ch] = jnp.where(
                place == cols - 1, right, pltpu.roll(value, cols - 1, 0)
            ).astype(BF16)

    def conv(field, weight, start, count):
        total = None
        for a in range(3):
            piece = field[(start + a) * cols : (start + a + count) * cols, :]
            part = jnp.dot(piece, weight[a], preferred_element_type=F32)
            total = part if total is None else total + part
        return total

    def flip(source, target):
        for a in range(3):
            for b in range(3):
                target[a, b * ch : (b + 1) * ch, :] = source[2 - a, (2 - b) * ch : (3 - b) * ch, :].T

    def centre(field, weight, start, count, steps):
        total = None
        for a in steps:
            piece = field[(start + a) * cols : (start + a + count) * cols, mid]
            part = jnp.dot(piece, weight[a, mid, :], preferred_element_type=F32)
            total = part if total is None else total + part
        partial[start * cols : (start + count) * cols, :] = total

    def centres(field, weight):
        for start in range(0, rows, group):
            steps = (1, 2) if start == 0 else (0, 1) if start == rows - group else (0, 1, 2)
            centre(field, weight, start, group, steps)

    def conv_rest(field, weight, start, count):
        total = partial[start * cols : (start + count) * cols, :]
        for a in range(3):
            where = slice((start + a) * cols, (start + a + count) * cols)
            for b in (0, 2):
                lanes_b = slice(b * ch, (b + 1) * ch)
                total = total + jnp.dot(
                    field[where, lanes_b], weight[a, lanes_b, :], preferred_element_type=F32
                )
        if start in (0, rows - group):
            a = 0 if start == 0 else 2
            where = slice((start + a) * cols, (start + a + count) * cols)
            total = total + jnp.dot(field[where, mid], weight[a, mid, :], preferred_element_type=F32)
        return total

    def put_rows(field, start, count, value, sides):
        for k in range(count):
            part = value[k * cols : (k + 1) * cols]
            put_mid(field, start + 1 + k, part)
            if sides:
                put_sides(field, start + 1 + k, part)

    def middle(step, block):
        for start in range(group, rows - group, block):
            step(start, block)

    def outer(step, block):
        for base in (0, rows - group):
            for start in range(base, base + group, block):
                step(start, block)

    own_rows = pl.ds(pl.multiple_of(core * half, half), half)
    other_rows = pl.ds(pl.multiple_of((1 - core) * half, half), half)

    def chunk(px, py):
        return pl.ds(pl.multiple_of((px * 4 + py) * 16, 16), 16)

    my_chunk = chunk(x, y)

    pieces = [(0, 3 * a, 3) for a in range(3)] + [(1, t, 1) for t in range(9)]
    number = {piece: n for n, piece in enumerate(pieces)}

    def taps(piece):
        return slice(piece[1], piece[1] + piece[2])

    def lanes(piece):
        first = piece[1] % 3
        return slice(first * ch, (first + piece[2]) * ch)

    def pair_copy(piece):
        g, t, _ = piece
        return remote(
            grads.at[g, t // 3, other_rows, lanes(piece)], pair.at[g, t // 3, :, lanes(piece)],
            pair_sem.at[number[piece]], partner,
        )

    def settle(ref, sems):
        pltpu.make_async_copy(ref, ref, sems.at[0]).wait()
        pltpu.make_async_copy(ref, ref, sems.at[1]).wait()

    def grad_piece(g, a, field):
        for part in (slice(0, half), slice(half, ch)):
            grads[g, a, part, :] = jnp.dot(
                turned[part, :], field[a * cols : (a + rows) * cols, :], preferred_element_type=F32
            )
        for piece in pieces:
            if piece[0] == g and piece[1] // 3 == a:
                pair_copy(piece).start()

    def scatter(piece):
        g, first, count = piece
        pair_copy(piece).wait()
        for t in range(first, first + count):
            a, b = t // 3, t % 3
            where = slice(b * ch, (b + 1) * ch)
            total = (grads[g, a, own_rows, where] + pair[g, a, :, where]).T
            mine[g, t] = total
            out1[g, t] = total.astype(BF16)
        for n, shift in enumerate(plane):
            px, py = in_plane(*shift)
            remote(
                out1.at[g, taps(piece), chunk(px, py), :], in1.at[g, taps(piece), n],
                plane_sem.at[number[piece]], at(px, py, z, core),
            ).start()

    def depth(piece):
        g = piece[0]
        settle(in1.at[g, taps(piece)], plane_sem.at[number[piece]])
        total = mine[g, taps(piece), my_chunk, :]
        for n in range(15):
            total = total + in1[g, taps(piece), n].astype(F32)
        zin[g, taps(piece), z] = total.astype(BF16)
        for d in range(1, 8):
            place = zin.at[g, taps(piece), z]
            remote(place, place, z_sem.at[number[piece]], at(x, y, lax.rem(z + d, 8), core)).start()

    def spread(piece):
        g = piece[0]
        settle(zin.at[g, taps(piece), 0:7], z_sem.at[number[piece]])
        total = zin[g, taps(piece), 0].astype(F32)
        for n in range(1, 8):
            total = total + zin[g, taps(piece), n].astype(F32)
        final[g, core, taps(piece), my_chunk, :] = total.astype(BF16)
        place = final.at[g, core, taps(piece), my_chunk, :]
        for shift in plane:
            px, py = in_plane(*shift)
            remote(place, place, spread_sem.at[number[piece]], at(px, py, z, core)).start()

    def last_copy(piece):
        place = final.at[piece[0], core, taps(piece)]
        return remote(place, place, last_sem.at[number[piece]], partner)

    def join(piece):
        settle(in1.at[piece[0], taps(piece)], spread_sem.at[number[piece]])
        last_copy(piece).start()

    def finish(piece):
        last_copy(piece).wait()
        if piece[0] == 0:
            for c in range(2):
                o2_ref[taps(piece), :, c * half : (c + 1) * half] = final[0, c, taps(piece)].astype(F32)

    early, late = pieces[:3], pieces[3:]

    def each(step, some):
        for piece in some:
            step(piece)

    loads[0].wait()
    for row in range(rows):
        edge[0, row : row + 1] = in_ref[row, 0:16].astype(F32)[0:1]
        edge[1, row : row + 1] = in_ref[row, cols - 16 : cols].astype(F32)[15:16]
    pl.semaphore_wait(barrier, len(peers))
    send(0, xs)

    def load(row, carry):
        value = in_ref[row].astype(F32)
        put_mid(xs, row + 1, value, mark=False)
        put_sides(xs, row + 1, value)
        return carry

    lax.fori_loop(0, rows, load, 0)
    for copy in loads[1:]:
        copy.wait()
    flip(w1_ref, wt1)
    flip(w2_ref, wt2)

    def span(start, count):
        return slice(start * cols, (start + count) * cols)

    def first(start, count):
        value = conv_rest(xs, w1_ref, start, count)
        slope1[span(start, count), :] = value
        put_rows(acts, start, count, value * half_erf(value), False)

    centres(xs, w1_ref)
    receive_sides(0, xs)
    middle(first, B1)
    receive_ends(0, xs)
    outer(first, B1)
    send(1, acts)

    def fill(row, carry):
        where = pl.ds(pl.multiple_of(row * cols, cols), cols)
        slope1[where, :] = slope_of(slope1[where, :])
        put_sides(acts, row + 1, acts[line(row + 1), mid].astype(F32))
        return carry

    lax.fori_loop(0, rows, fill, 0)

    def second(start, count):
        value = conv_rest(acts, w2_ref, start, count)
        rate = cot_ref[start : start + count].astype(F32).reshape(count * cols, ch)
        delta = rate * slope_of(value)
        put_rows(d2s, start, count, delta, True)
        turned[:, span(start, count)] = delta.astype(BF16).T

    centres(acts, w2_ref)
    receive_sides(1, acts)
    middle(second, B2)
    receive_ends(1, acts)
    outer(second, B2)
    send(2, d2s)
    grad_piece(0, 0, acts)
    grad_piece(0, 1, acts)
    grad_piece(0, 2, acts)
    scatter(early[0])

    def third(start, count):
        value = conv(d2s, wt2, start, count)
        delta = value * slope1[span(start, count), :]
        put_rows(d1s, start, count, delta, False)
        turned[:, span(start, count)] = delta.astype(BF16).T

    receive_sides(2, d2s)
    middle(third, B3)
    scatter(early[1])
    scatter(early[2])
    receive_ends(2, d2s)
    outer(third, B3)
    send(3, d1s)
    grad_piece(1, 0, xs)
    grad_piece(1, 1, xs)
    each(scatter, late[:3])
    depth(early[0])
    grad_piece(1, 2, xs)
    each(scatter, late[3:6])
    depth(early[1])
    each(scatter, late[6:])
    for row in range(1, rows + 1):
        put_sides(d1s, row, d1s[line(row), mid].astype(F32))

    def fourth(start, count):
        value = conv(d1s, wt1, start, count)
        dx_ref[start : start + count] = value.astype(BF16).reshape(count, cols, ch)

    receive_sides(3, d1s)
    depth(early[2])
    middle(fourth, B4)
    receive_ends(3, d1s)
    outer(fourth, B4)
    each(depth, late[:3])
    spread(early[0])
    each(depth, late[3:6])
    spread(early[1])
    each(depth, late[6:])
    spread(early[2])
    each(spread, late)
    each(join, early)
    each(join, late[:3])
    each(finish, early)
    each(join, late[3:])
    each(finish, late)


def write_kernel(dx_ref, final, g2_ref, dx_out, o1_out, o2_out, wide, sems):
    half = final.shape[-1]
    copies = [
        pltpu.make_async_copy(g2_ref, o2_out, sems.at[9]),
        pltpu.make_async_copy(dx_ref, dx_out, sems.at[10]),
    ]
    for copy in copies:
        copy.start()
    for t in range(9):
        for c in range(2):
            wide[t, :, c * half : (c + 1) * half] = final[1, c, t].astype(F32)
        copies.append(pltpu.make_async_copy(wide.at[t], o1_out.at[t], sems.at[t]))
        copies[-1].start()
    for copy in copies:
        copy.wait()


def body(lats, lons, inputs, first_filter, second_filter, cotangent):
    rows, cols, ch = inputs.shape
    group = 4
    vmem = pl.BlockSpec(memory_space=pltpu.VMEM)
    hbm = pl.BlockSpec(memory_space=pltpu.HBM)
    cells = rows * cols
    half = ch // 2
    padded = pltpu.VMEM(((rows + 2) * cols, 3 * ch), BF16)
    dma = pltpu.SemaphoreType.DMA
    dx, final, o2 = pl.pallas_call(
        functools.partial(kernel, lats, lons, rows, cols, ch, group),
        out_shape=(
            jax.ShapeDtypeStruct((rows, cols, ch), BF16),
            jax.ShapeDtypeStruct((2, 2, 9, ch, half), BF16),
            jax.ShapeDtypeStruct((9, ch, ch), F32),
        ),
        in_specs=[hbm] * 4,
        out_specs=(vmem,) * 3,
        scratch_shapes=[
            pltpu.VMEM((rows, cols, ch), BF16),
            pltpu.VMEM((3, 3 * ch, ch), BF16),
            pltpu.VMEM((3, 3 * ch, ch), BF16),
            pltpu.VMEM((rows, cols, ch), BF16),
            pltpu.VMEM((3, 3 * ch, ch), BF16),
            pltpu.VMEM((3, 3 * ch, ch), BF16),
            padded, padded, padded, padded,
            pltpu.VMEM((cells, ch), F32),
            pltpu.VMEM((cells, ch), F32),
            pltpu.VMEM((ch, cells), BF16),
            pltpu.VMEM((2, rows, ch), F32),
            pltpu.VMEM((4, 2, rows, ch), BF16),
            pltpu.VMEM((4, 2, 3, rows, ch), BF16),
            pltpu.VMEM((2, 16 + rows, ch), F32),
            pltpu.VMEM((2, 3, ch, 3 * ch), F32),
            pltpu.VMEM((2, 3, half, 3 * ch), F32),
            pltpu.VMEM((2, 9, ch, half), F32),
            pltpu.VMEM((2, 9, ch, half), BF16),
            pltpu.VMEM((2, 9, 15, 16, half), BF16),
            pltpu.VMEM((2, 9, 8, 16, half), BF16),
            dma((4,)), dma((4, 8)), dma((4, 8)),
            dma((12, 2)), dma((12, 2)), dma((12, 2)), dma((12, 2)), dma((12, 2)),
        ],
        compiler_params=pltpu.CompilerParams(
            collective_id=0, has_side_effects=True, vmem_limit_bytes=VMEM_LIMIT
        ),
        name="stages",
    )(
        *(
            pltpu.with_memory_space_constraint(value, pltpu.HBM)
            for value in (
                inputs,
                first_filter.reshape(3, 3 * ch, ch),
                second_filter.reshape(3, 3 * ch, ch),
                cotangent,
            )
        )
    )
    dx, o1, o2 = pl.pallas_call(
        write_kernel,
        out_shape=(
            jax.ShapeDtypeStruct((rows, cols, ch), BF16),
            jax.ShapeDtypeStruct((9, ch, ch), F32),
            jax.ShapeDtypeStruct((9, ch, ch), F32),
        ),
        in_specs=[vmem] * 3,
        out_specs=(hbm,) * 3,
        scratch_shapes=[pltpu.VMEM((9, ch, ch), F32), dma((11,))],
        compiler_params=pltpu.CompilerParams(vmem_limit_bytes=12 * 1024 * 1024),
        name="write",
    )(dx, final, o2)
    return dx, o1.reshape(3, 3, ch, ch), o2.reshape(3, 3, ch, ch)


def solution(mesh):
    in_specs = (P("lat", "lon", None), P(), P(), P("lat", "lon", None))
    out_specs = (P("lat", "lon", None), P(), P())
    step = functools.partial(body, mesh.shape["lat"], mesh.shape["lon"])
    return jax.shard_map(step, mesh=mesh, in_specs=in_specs, out_specs=out_specs, check_vma=False)
```
